128 devices in a mesh: rep: 4 (over x), rows: 32 (over z, y, core).
Axes of the slice: x: 4, y: 4, z: 4, core: 2. Of those that a mesh axis runs over, the one named last changes fastest.
Arguments:
- node_feat: bfloat16 [131072, 50], P(('rows', 'rep'))
- degree: int32 [131072], P(('rows', 'rep'))
- nbr_col: int32 [131072, 32], P('rows', 'rep')
- nbr_wt: bfloat16 [131072, 32], P('rows', 'rep')
- nbr_mask: int32 [131072, 32], P('rows', 'rep')
- w_one: bfloat16 [50, 2048], replicated
- w_two: bfloat16 [2048, 2048], replicated
- w_three: bfloat16 [2048, 121], replicated
Outputs:
- output: float32 [131072, 121], P(('rows', 'rep'))
All inputs are finite; a program needn't handle non-finite values.
Results may differ from the reference program's by a relative error of at most 0.001.
Values are sent between devices in bfloat16 or wider.
A program may use at most 1 GiB of HBM per device.

```python
import jax
import jax.numpy as jnp
from jax import lax

NODES_DEV = 1024
REP_SIZE = 4
ROW_GROUPS = 32
F_IN = 50
HID = 2048
CLS = 121
NBR = 32

NODES = NODES_DEV * REP_SIZE * ROW_GROUPS
RANGE_NBR = NBR // REP_SIZE
ROW_BLOCK = min(NODES_DEV, 512)


def draw_graph(graph_key):
    k_cnt, k_hub, k_grp, k_loc_a, k_loc_b = jax.random.split(graph_key, 5)
    counts = jax.random.randint(k_cnt, (NODES, REP_SIZE), 1, RANGE_NBR + 1)
    hub_range = jax.random.randint(k_hub, (), 0, REP_SIZE)
    counts = jnp.where(jnp.arange(REP_SIZE)[None, :] == hub_range, RANGE_NBR, counts)
    slot_ids = jnp.arange(RANGE_NBR)
    nbr_mask = (slot_ids[None, None, :] < counts[:, :, None]).astype(jnp.int32)
    table_shape = (NODES, REP_SIZE, RANGE_NBR)
    groups = jax.random.randint(k_grp, table_shape, 0, ROW_GROUPS)
    local_a = jax.random.randint(k_loc_a, table_shape, 0, NODES_DEV)
    local_b = jax.random.randint(k_loc_b, table_shape, 0, NODES_DEV)
    local_ids = (local_a * local_b) // NODES_DEV
    range_ids = jnp.arange(REP_SIZE)[None, :, None]
    nbr_col = (groups * REP_SIZE + range_ids) * NODES_DEV + local_ids
    degree = 1 + jnp.sum(counts, axis=1)
    return nbr_col.reshape(NODES, NBR).astype(jnp.int32), nbr_mask.reshape(NODES, NBR), degree.astype(jnp.int32)


def setup_inputs(seed: int = 0) -> dict:
    root_key = jax.random.key(seed)
    k_graph, k_feat, k_wt, k_one, k_two, k_three = jax.random.split(root_key, 6)
    nbr_col, nbr_mask, degree = draw_graph(k_graph)
    deg_mean = 1.0 + (NBR + REP_SIZE + RANGE_NBR) / 2.0
    node_feat = jax.random.normal(k_feat, (NODES, F_IN), jnp.float32)
    nbr_wt = jax.random.uniform(k_wt, (NODES, NBR), jnp.float32, 0.5, 1.5)
    w_one = jax.random.normal(k_one, (F_IN, HID), jnp.float32) * (deg_mean / F_IN) ** 0.5
    w_two = jax.random.normal(k_two, (HID, HID), jnp.float32) * (2.0 * deg_mean / HID) ** 0.5
    w_three = jax.random.normal(k_three, (HID, CLS), jnp.float32) * (2.0 * deg_mean / HID) ** 0.5
    return {'node_feat': node_feat.astype(jnp.bfloat16), 'degree': degree, 'nbr_col': nbr_col, 'nbr_wt': nbr_wt.astype(jnp.bfloat16), 'nbr_mask': nbr_mask, 'w_one': w_one.astype(jnp.bfloat16), 'w_two': w_two.astype(jnp.bfloat16), 'w_three': w_three.astype(jnp.bfloat16)}


def reference(node_feat, degree, nbr_col, nbr_wt, nbr_mask, w_one, w_two, w_three):
    inv_sqrt = lax.rsqrt(degree.astype(jnp.float32))[:, None]
    edge_wt = jnp.where(nbr_mask > 0, nbr_wt, jnp.zeros_like(nbr_wt))
    col_blocks = nbr_col.reshape(-1, ROW_BLOCK, NBR)
    wt_blocks = edge_wt.reshape(-1, ROW_BLOCK, NBR)

    def gcn_layer(hidden, w_mat):
        src_rows = (jnp.dot(hidden, w_mat, preferred_element_type=jnp.float32) * inv_sqrt).astype(jnp.bfloat16)

        def gather_sum(block_pair):
            blk_cols, blk_wts = block_pair
            picked = jnp.take(src_rows, blk_cols, axis=0)
            return jnp.einsum('nk,nkf->nf', blk_wts.astype(jnp.float32), picked.astype(jnp.float32))

        neigh_sum = lax.map(gather_sum, (col_blocks, wt_blocks)).reshape(NODES, -1)
        return inv_sqrt * (neigh_sum + src_rows.astype(jnp.float32))

    h_one = jnp.maximum(gcn_layer(node_feat, w_one), 0.0).astype(jnp.bfloat16)
    h_two = jnp.maximum(gcn_layer(h_one, w_two), 0.0).astype(jnp.bfloat16)
    return gcn_layer(h_two, w_three)
```

```python
import functools

import jax
import jax.numpy as jnp
from jax import lax
from jax.experimental import pallas as pl
from jax.experimental.pallas import tpu as pltpu
from jax.sharding import Mesh, PartitionSpec as P

LANES = 128
PAD = 8
GROUP = 1024
BUFS = 4


def gather_kernel(meta_ref, idx_hbm, wt_ref, src_hbm, *refs, phases, groups, blocked, from_feat, swap_core, finish):
    if from_feat:
        wbd_ref, deg_ref, out_ref, table, acc, stage, *rest = refs
    else:
        out_ref, table, acc, stage, *rest = refs
    sbufs, (sem_idx, sem_stage) = rest[:BUFS], rest[BUFS:]
    total = phases * groups
    n_blk = 32
    blk_rows = stage.shape[1]

    def stage_copy(p, b):
        src_b = (b % 16) * 2 + b // 16 if swap_core else b
        return pltpu.make_async_copy(src_hbm.at[p, src_b], stage.at[b], sem_stage.at[b])

    def idx_start(q):
        if blocked:
            p, gi = q // groups, q % groups
            return (((gi // 8) * phases + p) * 8 + gi % 8) * GROUP
        return q * GROUP

    def wt_index(p, gi):
        if blocked:
            return ((gi // 8) * (phases + 1) + p) * 8 + gi % 8
        return gi

    def idx_copy(q, b):
        return pltpu.make_async_copy(idx_hbm.at[pl.ds(pl.multiple_of(idx_start(q), GROUP), GROUP)], sbufs[b], sem_idx.at[b])

    for b in range(BUFS):
        idx_copy(b, b).start()

    def start_stage(p):
        def one(b, c):
            stage_copy(p, b).start()
            return c
        lax.fori_loop(0, n_blk, one, 0)

    start_stage(0)
    sub = lax.broadcasted_iota(jnp.int32, (8, LANES), 0)
    masks = [sub == j for j in range(8)]

    def zero(t, c):
        acc[pl.ds(pl.multiple_of(t * LANES, LANES), LANES), :] = jnp.zeros((LANES, LANES), jnp.float32)
        return c
    lax.fori_loop(0, acc.shape[0] // LANES, zero, 0)

    def phase(p, carry):
        def build(b, c):
            stage_copy(p, b).wait()
            r0 = pl.multiple_of(PAD + b * 1024, 8)
            if from_feat:
                x = stage[b]
                h = jnp.dot(x, wbd_ref[...], preferred_element_type=jnp.float32)
                d = jnp.dot(x, deg_ref[...], preferred_element_type=jnp.float32)
                v = (h * lax.rsqrt(d)).astype(jnp.bfloat16).astype(jnp.float32)
                table[pl.ds(r0, 512), :] = v[:, :LANES]
                table[pl.ds(r0 + 512, 512), :] = v[:, LANES:]
            else:
                table[pl.ds(r0, 1024), :] = stage[b].astype(jnp.float32)
            return c
        lax.fori_loop(0, n_blk, build, 0)

        @pl.when(p + 1 < phases)
        def _():
            start_stage(p + 1)

        def quad(t, c):
            for b in range(BUFS):
                gi = t * BUFS + b
                q = p * groups + gi
                idx_copy(q, b).wait()
                sref = sbufs[b]
                w = wt_ref[wt_index(p, gi)].astype(jnp.float32)
                for o in range(16):
                    a = None
                    for k in range(8):
                        m = None
                        for j in range(8):
                            v = table[pl.ds(sref[o * 64 + k * 8 + j], 8), :]
                            m = v if m is None else jnp.where(masks[j], v, m)
                        e = m * jnp.broadcast_to(w[:, o * 8 + k:o * 8 + k + 1], (8, LANES))
                        a = e if a is None else a + e
                    r = pl.multiple_of(gi * 128 + o * 8, 8)
                    acc[pl.ds(r, 8), :] += a

                @pl.when(q + BUFS < total)
                def _():
                    idx_copy(q + BUFS, b).start()
            return c
        lax.fori_loop(0, groups // BUFS, quad, 0)

        if finish:
            @pl.when(p == meta_ref[0])
            def _():
                def own(t, c):
                    r = pl.multiple_of(t * LANES, LANES)
                    o = pl.multiple_of(PAD + meta_ref[1] * (groups * LANES) + r, 8)
                    acc[pl.ds(r, LANES), :] += table[pl.ds(o, LANES), :]
                    return c
                lax.fori_loop(0, groups, own, 0)
        return carry
    lax.fori_loop(0, phases, phase, 0)

    if finish:
        def close(gi, c):
            s = lax.rsqrt(wt_ref[wt_index(phases, gi)].astype(jnp.float32))
            for o in range(0, 16, 2):
                r = pl.multiple_of(gi * 128 + o * 8, 16)
                sb = jnp.concatenate([jnp.broadcast_to(s[:, o + t:o + t + 1], (8, LANES)) for t in range(2)], axis=0)
                out_ref[pl.ds(r, 16), :] = jnp.maximum(acc[pl.ds(r, 16), :] * sb, 0.0).astype(jnp.bfloat16)
            return c
        lax.fori_loop(0, groups, close, 0)
    else:
        def close(t, c):
            r = pl.multiple_of(t * LANES, LANES)
            out_ref[pl.ds(r, LANES), :] = acc[pl.ds(r, LANES), :]
            return c
        lax.fori_loop(0, groups, close, 0)


def gather_call(meta, idx, wt, src, extra=(), *, phases, groups, blocked, from_feat, swap_core, finish, name):
    vm = pl.BlockSpec(memory_space=pltpu.VMEM)
    hb = pl.BlockSpec(memory_space=pl.ANY)
    rows = groups * LANES
    blk = src.shape[2]
    kern = functools.partial(gather_kernel, phases=phases, groups=groups, blocked=blocked, from_feat=from_feat, swap_core=swap_core, finish=finish)
    return pl.pallas_call(
        kern,
        out_shape=jax.ShapeDtypeStruct((rows, LANES), jnp.bfloat16 if finish else jnp.float32),
        in_specs=[pl.BlockSpec(memory_space=pltpu.SMEM), hb, vm, hb] + [vm] * len(extra),
        out_specs=vm,
        scratch_shapes=[
            pltpu.VMEM((PAD + 32768 + 8, LANES), jnp.float32),
            pltpu.VMEM((rows, LANES), jnp.float32),
            pltpu.VMEM((32, blk, LANES), jnp.bfloat16),
            *[pltpu.SMEM((GROUP,), jnp.int32) for _ in range(BUFS)],
            pltpu.SemaphoreType.DMA((BUFS,)),
            pltpu.SemaphoreType.DMA((32,)),
        ],
        compiler_params=pltpu.CompilerParams(vmem_limit_bytes=60 * 2**20),
        cost_estimate=pl.CostEstimate(flops=phases * groups * 2000000, bytes_accessed=2**25, transcendentals=0),
        name=name,
    )(meta, idx, wt, src, *extra)


def solution(mesh):
    mesh4 = Mesh(mesh.devices.reshape(4, 4, 4, 2), ('rep', 'z', 'y', 'core'))

    def device_body(node_feat, degree, nbr_col, nbr_wt, nbr_mask, w_one, w_two, w_three):
        bf = jnp.bfloat16
        nodes, f_in = node_feat.shape
        hid, cls = w_three.shape
        rep, core = lax.axis_index('rep'), lax.axis_index('core')
        fgroup = lax.axis_index('z') * 4 + lax.axis_index('y')
        inv_sqrt = lax.rsqrt(degree.astype(jnp.float32))[:, None]
        meta = jnp.stack([rep, core]).astype(jnp.int32)

        half = jnp.concatenate([node_feat, degree.astype(bf)[:, None], jnp.zeros((nodes, 64 - f_in - 1), bf)], axis=1)
        packed = jnp.concatenate([half[:nodes // 2], half[nodes // 2:]], axis=1)
        feats = lax.all_gather(packed, ('rep', 'z', 'y', 'core'), axis=0).reshape(4, 32, nodes // 2, LANES)

        blk = nbr_col // (4 * nodes)
        pos = ((blk % 2) * 16 + blk // 2) * nodes + nbr_col % nodes
        pos = pos + PAD - (jnp.arange(4 * nodes) % 8)[:, None]
        idx_own = pos.reshape(-1, 8, 8).transpose(0, 2, 1).reshape(-1)
        edge_wt = jnp.where(nbr_mask > 0, nbr_wt, jnp.zeros_like(nbr_wt))
        wt_own = edge_wt.reshape(-1, 16, 8, 8).transpose(0, 2, 1, 3).reshape(-1, 8, LANES)
        idx_all = lax.all_gather(lax.all_to_all(idx_own.reshape(4, -1), 'rep', 0, 0), ('z', 'y'), axis=0).reshape(-1)
        deg_own = degree.astype(bf).reshape(1, -1, 16, 8).transpose(0, 1, 3, 2)
        deg_own = jnp.pad(deg_own, ((0, 0), (0, 0), (0, 0), (0, LANES - 16)), constant_values=1)
        wt_mine = lax.all_to_all(wt_own.reshape(4, -1, 8, LANES), 'rep', 0, 0)
        wt_all = lax.all_gather(jnp.concatenate([wt_mine, deg_own], axis=0), ('z', 'y'), axis=0).reshape(-1, 8, LANES)

        w_loc = lax.dynamic_slice_in_dim(w_one, fgroup * LANES, LANES, axis=1)
        wbd = jnp.zeros((LANES, 2 * LANES), bf).at[:f_in, :LANES].set(w_loc).at[64:64 + f_in, LANES:].set(w_loc)
        ebd = jnp.zeros((LANES, 2 * LANES), bf).at[f_in, :LANES].set(1).at[64 + f_in, LANES:].set(1)

        def back(h):
            parts = lax.all_to_all(h.reshape(16, nodes, LANES), ('z', 'y'), 0, 0)
            return parts.transpose(1, 0, 2).reshape(nodes, hid)

        h_one = back(gather_call(meta, idx_all, wt_all, feats, (wbd, ebd), phases=4, groups=128, blocked=True, from_feat=True,
                                 swap_core=True, finish=True, name='layer_one'))
        s_two = (jnp.dot(h_one, w_two, preferred_element_type=jnp.float32) * inv_sqrt).astype(bf)
        s_two = lax.all_to_all(s_two.reshape(nodes, 16, LANES).transpose(1, 0, 2), ('z', 'y'), 0, 0)
        s_two = lax.all_gather(s_two, ('rep', 'core'), axis=0).reshape(4, 32, nodes, LANES)
        h_two = back(gather_call(meta, idx_all, wt_all, s_two, phases=4, groups=128, blocked=True, from_feat=False,
                                 swap_core=False, finish=True, name='layer_two'))
        w_pad = jnp.pad(w_three, ((0, 0), (0, LANES - cls)))
        s_three = (jnp.dot(h_two, w_pad, preferred_element_type=jnp.float32) * inv_sqrt).astype(bf)
        s_all = lax.all_gather(s_three, ('z', 'y', 'core'), axis=0).reshape(1, 32, nodes, LANES)
        part = gather_call(meta, idx_own, wt_own, s_all, phases=1, groups=32, blocked=False, from_feat=False,
                           swap_core=True, finish=False, name='layer_three')
        neigh = lax.psum_scatter(part, 'rep', scatter_dimension=0, tiled=True)
        return (inv_sqrt * (neigh + s_three.astype(jnp.float32)))[:, :cls]

    rows = ('z', 'y', 'core')
    row_spec = P((*rows, 'rep'), None)
    table_spec = P(rows, 'rep')
    full = P(None, None)
    return jax.shard_map(device_body, mesh=mesh4, in_specs=(row_spec, P((*rows, 'rep')), table_spec, table_spec, table_spec, full, full, full),
                         out_specs=row_spec, check_vma=False)
```

```python
import functools

import jax
import jax.numpy as jnp
from jax import lax
from jax.experimental import pallas as pl
from jax.experimental.pallas import tpu as pltpu
from jax.experimental.layout import Layout, with_layout_constraint
from jax.sharding import Mesh, PartitionSpec as P

LANES = 128
PAD = 8
GROUP = 1024
BUFS = 4


class Plan:
    def __init__(self, name, phases, groups, sub, first, last):
        self.name, self.phases, self.groups, self.sub = name, phases, groups, sub
        self.first, self.last = first, last
        self.nodes = 8 // sub
        self.group_rows = GROUP // 8 * sub
        self.rows = groups * self.group_rows


def gather_kernel(plan, n_src, meta_ref, idx_ref, wt_ref, *refs):
    kind = plan.name
    srcs, refs = refs[:len(n_src)], refs[len(n_src):]
    w_ref = prev = None
    if kind == 'one':
        w_ref, refs = refs[0], refs[1:]
    if not plan.first:
        prev, refs = refs[0], refs[1:]
    out_ref, table, acc, stage, *refs = refs
    sbufs, (sem_idx, sem_stage, sem_acc) = refs[:BUFS], refs[BUFS:]
    groups, sub, n_ph = plan.groups, plan.sub, len(plan.phases)
    total = n_ph * groups
    rep, core, zy = meta_ref[0], meta_ref[1], meta_ref[2]

    def col_set(ph):
        d = plan.phases[0]
        for k in range(1, n_ph):
            d = jnp.where(ph == k, plan.phases[k], d)
        return (rep + d) % 4

    def idx_start(q):
        ph, gi = q // groups, q % groups
        if kind == 'one':
            nb, k = gi // 8, gi % 8
            return (((col_set(ph) * 2 + nb % 2) * 4 + nb // 2) * 8 + k) * GROUP
        if kind == 'two':
            return (((gi // 8) * 4 + col_set(ph)) * 8 + gi % 8) * GROUP
        return gi * GROUP

    def wt_index(ph, gi):
        if kind == 'one':
            nb, k = gi // 8, gi % 8
            return (col_set(ph) * 2 + nb % 2) * 72 + ((nb // 2) * 8 + k) * 2
        if kind == 'two':
            return ((gi // 8) * 5 + col_set(ph)) * 8 + gi % 8
        return gi

    def deg_index(gi):
        if kind == 'one':
            return (gi // 8) * 72 + 64 + gi % 8
        return ((gi // 8) * 5 + 4) * 8 + gi % 8

    def idx_copy(q, b):
        return pltpu.make_async_copy(idx_ref.at[pl.ds(pl.multiple_of(idx_start(q), GROUP), GROUP)], sbufs[b], sem_idx.at[b])

    def start_stage(ph):
        if kind == 'two':
            mine = [t for t, owner in zip(srcs, n_src) if owner == ph]
            per = 32 // len(mine)
            for h, src in enumerate(mine):
                def one(b, c):
                    pltpu.make_async_copy(src.at[b], stage.at[h * per + b], sem_stage.at[h * per + b]).start()
                    return c
                lax.fori_loop(0, per, one, 0)
            return

        def each(b, c):
            if kind == 'one':
                src = srcs[0].at[col_set(ph), (b % 16) * 2 + b // 16]
            else:
                src = srcs[0].at[(b % 16) * 2 + lax.rem(b // 16 + core, 2)]
            pltpu.make_async_copy(src, stage.at[b], sem_stage.at[b]).start()
            return c
        lax.fori_loop(0, 32, each, 0)

    for b in range(BUFS):
        idx_copy(b, b).start()
    start_stage(0)
    if plan.first:
        def zero(t, c):
            acc[pl.ds(pl.multiple_of(t * LANES, LANES), LANES), :] = jnp.zeros((LANES, LANES), jnp.float32)
            return c
        lax.fori_loop(0, plan.rows // LANES, zero, 0)
    else:
        load = pltpu.make_async_copy(prev, acc, sem_acc)
        load.start()
        load.wait()

    masks = [lax.broadcasted_iota(jnp.int32, (8, LANES), 0) // sub == j for j in range(plan.nodes)]

    def add_own(a_off, t_off, n):
        def own(t, c):
            r = pl.multiple_of(a_off + t * LANES, LANES)
            o = pl.multiple_of(PAD + t_off + t * LANES, 8)
            acc[pl.ds(r, LANES), :] += table[pl.ds(o, LANES), :]
            return c
        lax.fori_loop(0, n // LANES, own, 0)

    def phase(ph, carry):
        def build(b, c):
            pltpu.make_async_copy(stage.at[b], stage.at[b], sem_stage.at[b]).wait()
            r0 = pl.multiple_of(PAD + b * (1024 * sub), 8)
            if kind == 'one':
                x = stage[b]
                n = x.shape[0]
                h = jnp.dot(x, w_ref[...], preferred_element_type=jnp.float32)
                for a in range(2):
                    d = x[:, a * 64 + 50:a * 64 + 51].astype(jnp.float32)
                    s = lax.rsqrt(jnp.broadcast_to(d, (n, LANES)))
                    for f in range(2):
                        v = (h[:, (a * 2 + f) * LANES:(a * 2 + f + 1) * LANES] * s).astype(jnp.bfloat16).astype(jnp.float32)
                        table[pl.ds(r0 + a * (2 * n) + f, n, stride=2), :] = v
            else:
                table[pl.ds(r0, 1024), :] = stage[b].astype(jnp.float32)
            return c
        lax.fori_loop(0, 32, build, 0)

        if kind == 'two':
            for k in range(1, n_ph):
                @pl.when(ph + 1 == k)
                def _():
                    start_stage(k)
        elif n_ph > 1:
            @pl.when(ph + 1 < n_ph)
            def _():
                start_stage(ph + 1)

        if kind == 'one':
            for c2 in range(2):
                add_own((col_set(ph) * 2 + c2) * 2048, (c2 * 16 + zy) * 2048, 2048)
        elif kind == 'two' and plan.first:
            add_own(0, 0, plan.rows)

        def quad(t, c):
            for b in range(BUFS):
                gi = t * BUFS + b
                q = ph * groups + gi
                idx_copy(q, b).wait()
                sref = sbufs[b]
                wi = wt_index(ph, gi)
                for o in range(16 * sub):
                    if o % 16 == 0:
                        w = wt_ref[wi + o // 16].astype(jnp.float32)
                    a = None
                    for k in range(8):
                        m = None
                        for j in range(plan.nodes):
                            v = table[pl.ds(sref[(o * 8 + k) * plan.nodes + j], 8), :]
                            m = v if m is None else jnp.where(masks[j], v, m)
                        lane = (o % 16) * 8 + k
                        e = m * jnp.broadcast_to(w[:, lane:lane + 1], (8, LANES))
                        a = e if a is None else a + e
                    r = pl.multiple_of(gi * plan.group_rows + o * 8, 8)
                    acc[pl.ds(r, 8), :] += a

                @pl.when(q + BUFS < total)
                def _():
                    idx_copy(q + BUFS, b).start()
            return c
        lax.fori_loop(0, groups // BUFS, quad, 0)
        return carry
    lax.fori_loop(0, n_ph, phase, 0)

    if not plan.last:
        save = pltpu.make_async_copy(acc, out_ref, sem_acc)
        save.start()
        save.wait()
        return

    def close(gi, c):
        s = lax.rsqrt(wt_ref[deg_index(gi)].astype(jnp.float32))
        for o in range(0, 16, 2):
            sb = jnp.concatenate([jnp.broadcast_to(s[:, o + t:o + t + 1], (8, LANES)) for t in range(2)], axis=0)
            r = pl.multiple_of(gi * 128 + o * 8, 16)
            for f in range(sub):
                z = acc[pl.ds(gi * plan.group_rows + o * 8 * sub + f, 16, stride=sub), :] if sub > 1 else acc[pl.ds(r, 16), :]
                out_ref[pl.ds(r, 16), f * LANES:(f + 1) * LANES] = jnp.maximum(z * sb, 0.0).astype(jnp.bfloat16)
        return c
    lax.fori_loop(0, groups, close, 0)


def gather_call(plan, meta, idx, wt, by_phase, extra=()):
    vm = pl.BlockSpec(memory_space=pltpu.VMEM)
    hb = pl.BlockSpec(memory_space=pl.ANY)
    srcs = [t for group in by_phase for t in group]
    owners = [ph for ph, group in enumerate(by_phase) for _ in group]
    blk = srcs[0].shape[-2]
    if plan.last:
        shape, spec = jax.ShapeDtypeStruct((plan.rows // plan.sub, plan.sub * LANES), jnp.bfloat16), vm
    else:
        shape, spec = jax.ShapeDtypeStruct((plan.rows, LANES), jnp.float32), hb
    extra_specs = ([vm] if plan.name == 'one' else []) + ([] if plan.first else [hb])
    return pl.pallas_call(
        functools.partial(gather_kernel, plan, owners),
        out_shape=shape,
        in_specs=[pl.BlockSpec(memory_space=pltpu.SMEM), vm, vm] + [hb] * len(srcs) + extra_specs,
        out_specs=spec,
        scratch_shapes=[
            pltpu.VMEM((PAD + 32768 * plan.sub + 8, LANES), jnp.float32),
            pltpu.VMEM((plan.rows, LANES), jnp.float32),
            pltpu.VMEM((32, blk, LANES), jnp.bfloat16),
            *[pltpu.SMEM((GROUP,), jnp.int32) for _ in range(BUFS)],
            pltpu.SemaphoreType.DMA((BUFS,)),
            pltpu.SemaphoreType.DMA((32,)),
            pltpu.SemaphoreType.DMA,
        ],
        compiler_params=pltpu.CompilerParams(vmem_limit_bytes=60 * 2**20),
        cost_estimate=pl.CostEstimate(flops=len(plan.phases) * plan.groups * 100000000, bytes_accessed=2**25, transcendentals=0),
        name='gather_' + plan.name + str(plan.phases[0]),
    )(meta, idx, wt, *srcs, *extra)


def project_kernel(parts_ref, w_ref, s_ref, out_ref, rows):
    @pl.when(pl.program_id(0) == 0)
    def _():
        for g in range(8):
            rows[:, g * 256:(g + 1) * 256] = parts_ref[g]
    for t in range(4):
        r = slice(t * 256, (t + 1) * 256)
        v = jnp.dot(rows[r, :], w_ref[...], preferred_element_type=jnp.float32)
        for f in range(2):
            out_ref[f, r, :] = (v[:, f * LANES:(f + 1) * LANES] * s_ref[r, :]).astype(jnp.bfloat16)


def project_call(parts, w, s):
    nodes, hid = parts.shape[1], w.shape[1]
    whole = lambda shape: pl.BlockSpec(shape, lambda t: (0,) * len(shape))
    return pl.pallas_call(
        project_kernel,
        grid=(hid // 256,),
        out_shape=jax.ShapeDtypeStruct((hid // LANES, nodes, LANES), jnp.bfloat16),
        in_specs=[whole(parts.shape), pl.BlockSpec((w.shape[0], 256), lambda t: (0, t)), whole((nodes, LANES))],
        out_specs=pl.BlockSpec((2, nodes, LANES), lambda t: (t, 0, 0)),
        scratch_shapes=[pltpu.VMEM((nodes, w.shape[0]), jnp.bfloat16)],
        compiler_params=pltpu.CompilerParams(vmem_limit_bytes=40 * 2**20),
        cost_estimate=pl.CostEstimate(flops=2 * nodes * hid * hid, bytes_accessed=2**24, transcendentals=0),
        name='project',
    )(parts, w, s)


def solution(mesh):
    mesh4 = Mesh(mesh.devices.reshape(4, 4, 4, 2), ('rep', 'z', 'y', 'core'))
    shift = {d: [((t + d) % 4, t) for t in range(4)] for d in (1, 3)}
    swap = [(0, 1), (1, 0)]

    def device_body(node_feat, degree, nbr_col, nbr_wt, nbr_mask, w_one, w_two, w_three):
        bf = jnp.bfloat16
        nodes, f_in = node_feat.shape
        hid, cls = w_three.shape
        rep, core = lax.axis_index('rep'), lax.axis_index('core')
        zy = lax.axis_index('z') * 4 + lax.axis_index('y')
        inv_sqrt = lax.rsqrt(degree.astype(jnp.float32))[:, None]
        meta = jnp.stack([rep, core, zy]).astype(jnp.int32)

        half = jnp.concatenate([node_feat, degree.astype(bf)[:, None], jnp.zeros((nodes, 64 - f_in - 1), bf)], axis=1)
        packed = jnp.concatenate([half[:nodes // 2], half[nodes // 2:]], axis=1)
        packed = with_layout_constraint(packed, Layout((0, 1)))
        feats = lax.all_gather(packed, ('rep', 'z', 'y', 'core'), axis=0).reshape(4, 32, nodes // 2, LANES)

        def spread(x, axes, size):
            return lax.all_to_all(jnp.broadcast_to(x[None], (size, *x.shape)), axes, 0, 0)

        blk = nbr_col // (4 * nodes)
        inner = (blk // 2) * nodes + nbr_col % nodes
        lane_id = jnp.arange(4 * nodes)[:, None]
        pos_one = ((blk % 2) * (16 * nodes) + inner - lane_id % 4) * 2 + PAD
        pos_two = ((blk + core) % 2) * (16 * nodes) + inner - lane_id % 8 + PAD
        edge_wt = jnp.where(nbr_mask > 0, nbr_wt, jnp.zeros_like(nbr_wt))
        deg_own = degree.astype(bf).reshape(-1, 16, 8).transpose(0, 2, 1)
        deg_own = jnp.pad(deg_own, ((0, 0), (0, 0), (0, LANES - 16)), constant_values=1)

        idx_one = spread(pos_one.reshape(-1, 4, 8).transpose(0, 2, 1).reshape(-1), ('rep', 'core'), 8).reshape(-1)
        wt_q = jnp.repeat(edge_wt.reshape(-1, 16, 4, 8).transpose(0, 2, 1, 3).reshape(-1, 4, LANES), 2, axis=1)
        wt_one = spread(jnp.concatenate([wt_q, deg_own], axis=0), ('rep', 'core'), 8).reshape(-1, 8, LANES)

        idx_own = pos_two.reshape(-1, 8, 8).transpose(0, 2, 1).reshape(-1)
        wt_own = edge_wt.reshape(-1, 16, 8, 8).transpose(0, 2, 1, 3).reshape(-1, 8, LANES)
        idx_mine = lax.all_to_all(idx_own.reshape(4, -1), 'rep', 0, 0).reshape(-1)
        wt_mine = lax.all_to_all(wt_own.reshape(4, -1, 8, LANES), 'rep', 0, 0).reshape(-1, 8, LANES)
        feats, idx_one, wt_one, idx_mine, wt_mine = lax.optimization_barrier((feats, idx_one, wt_one, idx_mine, wt_mine))
        idx_two = lax.all_gather(idx_mine, ('z', 'y'), axis=0).reshape(-1)
        wt_two = lax.all_gather(jnp.concatenate([wt_mine, deg_own], axis=0), ('z', 'y'), axis=0).reshape(-1, 8, LANES)

        w_loc = lax.dynamic_slice_in_dim(w_one, (rep * 2 + core) * 256, 256, axis=1)
        wbd = jnp.zeros((LANES, 512), bf).at[:f_in, :256].set(w_loc).at[64:64 + f_in, 256:].set(w_loc)

        h = gather_call(Plan('one', (0, 1, 3, 2), 64, 2, True, True), meta, idx_one, wt_one, ((feats,),), (wbd,))
        h, idx_two, wt_two = lax.optimization_barrier((h, idx_two, wt_two))
        h = lax.all_to_all(h.reshape(8, nodes, 256), ('rep', 'core'), 0, 0)

        s_two = project_call(h, w_two, jnp.broadcast_to(inv_sqrt, (nodes, LANES)))
        t_0 = lax.all_to_all(s_two, ('z', 'y'), 0, 0)
        t_1, t_3 = (lax.ppermute(t_0, 'rep', shift[d]) for d in (1, 3))
        other = lambda t: lax.ppermute(t, 'core', swap)
        a = gather_call(Plan('two', (0,), 128, 1, True, False), meta, idx_two, wt_two, ((t_0, other(t_0)),))
        a, t_1, t_3 = lax.optimization_barrier((a, t_1, t_3))
        t_2 = [lax.ppermute(t_1[:8], 'rep', shift[1]), lax.ppermute(t_3[8:], 'rep', shift[3])]
        a = gather_call(Plan('two', (1, 3), 128, 1, False, False), meta, idx_two, wt_two, ((t_1, other(t_1)), (t_3, other(t_3))), (a,))
        a, *t_2 = lax.optimization_barrier((a, *t_2))
        h = gather_call(Plan('two', (2,), 128, 1, False, True), meta, idx_two, wt_two, ((*t_2, *map(other, t_2)),), (a,))
        h = lax.all_to_all(h.reshape(16, nodes, LANES), ('z', 'y'), 0, 0).transpose(1, 0, 2).reshape(nodes, hid)

        w_pad = jnp.pad(w_three, ((0, 0), (0, LANES - cls)))
        s_three = (jnp.dot(h, w_pad, preferred_element_type=jnp.float32) * inv_sqrt).astype(bf)
        s_all = lax.all_gather(s_three, ('z', 'y', 'core'), axis=0).reshape(32, nodes, LANES)
        part = gather_call(Plan('three', (0,), 32, 1, True, False), meta, idx_own, wt_own, ((s_all,),))
        neigh = lax.psum_scatter(part, 'rep', scatter_dimension=0, tiled=True)
        return (inv_sqrt * (neigh + s_three.astype(jnp.float32)))[:, :cls]

    rows = ('z', 'y', 'core')
    row_spec = P((*rows, 'rep'), None)
    table_spec = P(rows, 'rep')
    full = P(None, None)
    return jax.shard_map(device_body, mesh=mesh4, in_specs=(row_spec, P((*rows, 'rep')), table_spec, table_spec, table_spec, full, full, full),
                         out_specs=row_spec, check_vma=False)
```

```python
import functools

import jax
import jax.numpy as jnp
from jax import lax
from jax.experimental import pallas as pl
from jax.experimental.pallas import tpu as pltpu
from jax.experimental.layout import Layout, with_layout_constraint
from jax.sharding import Mesh, PartitionSpec as P

LANES = 128
PAD = 8
UNIT = 1024
BUFS = 2


class Plan:
    def __init__(self, name, phases, groups, sub, first, last, half=None):
        self.name, self.phases, self.groups, self.sub = name, phases, groups, sub
        self.first, self.last, self.half = first, last, half
        self.step = sub
        self.nodes = 8 // sub
        self.group_rows = UNIT // 8 * sub
        self.rows = groups * self.group_rows


def gather_kernel(plan, n_src, meta_ref, idx_ref, wt_ref, *refs):
    kind = plan.name
    srcs, refs = refs[:len(n_src)], refs[len(n_src):]
    w_ref = prev = None
    if kind == 'one':
        w_ref, refs = refs[0], refs[1:]
    if not plan.first:
        prev, refs = refs[0], refs[1:]
    out_ref, table, acc, stage, *refs = refs
    sbufs, (sem_idx, sem_stage, sem_acc) = refs[:BUFS], refs[BUFS:]
    groups, sub, n_ph = plan.groups, plan.sub, len(plan.phases)
    step = plan.step
    total = n_ph * groups // step
    rep, core, zy = meta_ref[0], meta_ref[1], meta_ref[2]

    def offset(ph):
        d = plan.phases[0]
        for k in range(1, n_ph):
            d = jnp.where(ph == k, plan.phases[k], d)
        return d

    def col_set(ph):
        return (rep + offset(ph)) % 4

    def unit_of(gi):
        if plan.half is None:
            return gi // 8, gi % 8
        return gi // 4, plan.half * 4 + gi % 4

    def idx_start(q):
        ph, gi = (q * step) // groups, (q * step) % groups
        nb, k = unit_of(gi)
        if kind == 'one':
            return (((offset(ph) * 2 + nb % 2) * 4 + nb // 2) * 8 + k) * UNIT
        if kind == 'two':
            return ((nb * 4 + col_set(ph)) * 8 + k) * UNIT
        return gi * UNIT

    def wt_index(ph, gi):
        nb, k = unit_of(gi)
        if kind == 'one':
            return (offset(ph) * 2 + nb % 2) * 72 + ((nb // 2) * 8 + k) * 2
        if kind == 'two':
            return (nb * 5 + col_set(ph)) * 8 + k
        return gi

    def deg_index(gi):
        nb, k = unit_of(gi)
        if kind == 'one':
            return (((nb // 2 - rep + 4) % 4) * 2 + nb % 2) * 72 + 64 + k
        return (nb * 5 + 4) * 8 + k

    def idx_copy(q, b):
        return pltpu.make_async_copy(idx_ref.at[pl.ds(pl.multiple_of(idx_start(q), UNIT), UNIT * step)], sbufs[b], sem_idx.at[b])

    def start_stage(ph):
        if kind == 'two':
            mine = [t for t, owner in zip(srcs, n_src) if owner == ph]
            per = 32 // len(mine)
            for h, src in enumerate(mine):
                def one(b, c):
                    pltpu.make_async_copy(src.at[b], stage.at[h * per + b], sem_stage.at[h * per + b]).start()
                    return c

                lax.fori_loop(0, per, one, 0)
            return

        def each(b, c):
            if kind == 'one':
                src_b = (b % 16) * 2 + b // 16
                src = srcs[0].at[src_b] if plan.first else srcs[0].at[col_set(ph), src_b]
                pltpu.make_async_copy(src, stage.at[b], sem_stage.at[b]).start()
            else:
                src_b = (b % 16) * 2 + lax.rem(b // 16 + core, 2)
                pltpu.make_async_copy(srcs[0].at[src_b], stage.at[b], sem_stage.at[b]).start()
            return c

        lax.fori_loop(0, 32, each, 0)

    for b in range(BUFS):
        idx_copy(b, b).start()
    start_stage(0)
    if plan.first:
        def zero(t, c):
            acc[pl.ds(pl.multiple_of(t * LANES, LANES), LANES), :] = jnp.zeros((LANES, LANES), jnp.float32)
            return c

        lax.fori_loop(0, plan.rows // LANES, zero, 0)
    else:
        if plan.half is None:
            pltpu.make_async_copy(prev, acc, sem_acc).start()
        else:
            def load(b, c):
                pltpu.make_async_copy(prev.at[b, plan.half], acc.at[pl.ds(pl.multiple_of(b * 512, 512), 512)], sem_acc).start()
                return c

            lax.fori_loop(0, 16, load, 0)
        pltpu.make_async_copy(acc, acc, sem_acc).wait()

    masks = [lax.broadcasted_iota(jnp.int32, (8, LANES), 0) // sub == j for j in range(plan.nodes)]

    def add_own(a_off, t_off, n):
        def own(t, c):
            r = pl.multiple_of(a_off + t * LANES, LANES)
            o = pl.multiple_of(PAD + t_off + t * LANES, 8)
            acc[pl.ds(r, LANES), :] += table[pl.ds(o, LANES), :]
            return c

        lax.fori_loop(0, n // LANES, own, 0)

    def phase(ph, carry):
        def build(b, c):
            pltpu.make_async_copy(stage.at[b], stage.at[b], sem_stage.at[b]).wait()
            r0 = pl.multiple_of(PAD + b * (1024 * sub), 8)
            if kind == 'one':
                x = stage[b]
                n = x.shape[0]
                h = jnp.dot(x, w_ref[...], preferred_element_type=jnp.float32)
                for a in range(2):
                    d = x[:, a * 64 + 50:a * 64 + 51].astype(jnp.float32)
                    s = lax.rsqrt(jnp.broadcast_to(d, (n, LANES)))
                    for f in range(2):
                        v = (h[:, (a * 2 + f) * LANES:(a * 2 + f + 1) * LANES] * s).astype(jnp.bfloat16).astype(jnp.float32)
                        table[pl.ds(r0 + a * (2 * n) + f, n, stride=2), :] = v
            else:
                table[pl.ds(r0, 1024), :] = stage[b].astype(jnp.float32)
            return c

        lax.fori_loop(0, 32, build, 0)

        if kind == 'two':
            for k in range(1, n_ph):
                @pl.when(ph + 1 == k)
                def _():
                    start_stage(k)
        elif n_ph > 1:
            @pl.when(ph + 1 < n_ph)
            def _():
                start_stage(ph + 1)

        if kind == 'one':
            for c2 in range(2):
                add_own((col_set(ph) * 2 + c2) * 2048, (c2 * 16 + zy) * 2048, 2048)
        elif kind == 'two' and plan.first:
            add_own(0, 0, plan.rows)

        def quad(t, c):
            for b in range(BUFS):
                gq = t * BUFS + b
                q = ph * (groups // step) + gq
                idx_copy(q, b).wait()
                sref = sbufs[b]
                for u in range(step):
                    gi = gq * step + u
                    wi = wt_index(ph, gi)
                    for o in range(16 * sub):
                        if o % 16 == 0:
                            w = wt_ref[wi + o // 16].astype(jnp.float32)
                        r = pl.multiple_of(gi * plan.group_rows + o * 8, 8)
                        a = acc[pl.ds(r, 8), :]
                        for k in range(8):
                            m = None
                            for j in range(plan.nodes):
                                v = table[pl.ds(sref[u * UNIT + k * 128 + o * plan.nodes + j], 8), :]
                                m = v if m is None else jnp.where(masks[j], v, m)
                            lane = (o % 16) * 8 + k
                            e = m * jnp.broadcast_to(w[:, lane:lane + 1], (8, LANES))
                            a = e if a is None else a + e
                        acc[pl.ds(r, 8), :] = a

                @pl.when(q + BUFS < total)
                def _():
                    idx_copy(q + BUFS, b).start()
            return c

        lax.fori_loop(0, groups // (step * BUFS), quad, 0)
        return carry

    lax.fori_loop(0, n_ph, phase, 0)

    if not plan.last:
        save = pltpu.make_async_copy(acc, out_ref, sem_acc)
        save.start()
        save.wait()
        return

    def close(gi, c):
        s = lax.rsqrt(wt_ref[deg_index(gi)].astype(jnp.float32))
        for o in range(0, 16, 2):
            sb = jnp.concatenate([jnp.broadcast_to(s[:, o + t:o + t + 1], (8, LANES)) for t in range(2)], axis=0)
            r = pl.multiple_of(gi * 128 + o * 8, 16)
            for f in range(sub):
                z = acc[pl.ds(gi * plan.group_rows + o * 8 * sub + f, 16, stride=sub), :] if sub > 1 else acc[pl.ds(r, 16), :]
                out_ref[pl.ds(r, 16), f * LANES:(f + 1) * LANES] = jnp.maximum(z * sb, 0.0).astype(jnp.bfloat16)
        return c

    lax.fori_loop(0, groups, close, 0)


def gather_call(plan, meta, idx, wt, by_phase, extra=()):
    vm = pl.BlockSpec(memory_space=pltpu.VMEM)
    hb = pl.BlockSpec(memory_space=pl.ANY)
    srcs = [t for group in by_phase for t in group]
    owners = [ph for ph, group in enumerate(by_phase) for _ in group]
    if plan.last:
        shape, spec = jax.ShapeDtypeStruct((plan.rows // plan.sub, plan.sub * LANES), jnp.bfloat16), vm
    else:
        shape, spec = jax.ShapeDtypeStruct((plan.rows, LANES), jnp.float32), hb
    extra_specs = ([vm] if plan.name == 'one' else []) + ([] if plan.first else [hb])
    return pl.pallas_call(
        functools.partial(gather_kernel, plan, owners),
        out_shape=shape,
        in_specs=[pl.BlockSpec(memory_space=pltpu.SMEM), vm, vm] + [hb] * len(srcs) + extra_specs,
        out_specs=spec,
        scratch_shapes=[
            pltpu.VMEM((PAD + 32768 * plan.sub + 8, LANES), jnp.float32),
            pltpu.VMEM((plan.rows, LANES), jnp.float32),
            pltpu.VMEM((32, 512 if plan.name == 'one' else 1024, LANES), jnp.bfloat16),
            *[pltpu.SMEM((UNIT * plan.step,), jnp.int32) for _ in range(BUFS)],
            pltpu.SemaphoreType.DMA((BUFS,)),
            pltpu.SemaphoreType.DMA((32,)),
            pltpu.SemaphoreType.DMA,
        ],
        compiler_params=pltpu.CompilerParams(vmem_limit_bytes=60 * 2**20),
        cost_estimate=pl.CostEstimate(flops=len(plan.phases) * plan.groups * 100000000, bytes_accessed=2**25, transcendentals=0),
    )(meta, idx, wt, *srcs, *extra)


def project_kernel(parts_ref, w_ref, s_ref, out_ref, rows):
    @pl.when(pl.program_id(0) == 0)
    def _():
        for g in range(8):
            rows[:, g * 256:(g + 1) * 256] = parts_ref[g]

    for t in range(4):
        r = slice(t * 256, (t + 1) * 256)
        v = jnp.dot(rows[r, :], w_ref[...], preferred_element_type=jnp.float32)
        for f in range(2):
            out_ref[f, r, :] = (v[:, f * LANES:(f + 1) * LANES] * s_ref[r, :]).astype(jnp.bfloat16)


def project_call(parts, w, s):
    nodes, hid = parts.shape[1], w.shape[1]
    whole = lambda shape: pl.BlockSpec(shape, lambda t: (0,) * len(shape))
    return pl.pallas_call(
        project_kernel,
        grid=(hid // 256,),
        out_shape=jax.ShapeDtypeStruct((hid // LANES, nodes, LANES), jnp.bfloat16),
        in_specs=[whole(parts.shape), pl.BlockSpec((w.shape[0], 256), lambda t: (0, t)), whole((nodes, LANES))],
        out_specs=pl.BlockSpec((2, nodes, LANES), lambda t: (t, 0, 0)),
        scratch_shapes=[pltpu.VMEM((nodes, w.shape[0]), jnp.bfloat16)],
        compiler_params=pltpu.CompilerParams(vmem_limit_bytes=40 * 2**20),
        cost_estimate=pl.CostEstimate(flops=2 * nodes * hid * hid, bytes_accessed=2**24, transcendentals=0),
        name='project',
    )(parts, w, s)


def solution(mesh):
    mesh4 = Mesh(mesh.devices.reshape(4, 4, 4, 2), ('rep', 'z', 'y', 'core'))
    shift = {d: [((t + d) % 4, t) for t in range(4)] for d in (1, 3)}
    swap = [(0, 1), (1, 0)]

    def network(node_feat, degree, nbr_col, nbr_wt, nbr_mask, w_one, w_two, w_three):
        bf = jnp.bfloat16
        nodes, f_in = node_feat.shape
        hid, cls = w_three.shape
        rep, core = lax.axis_index('rep'), lax.axis_index('core')
        zy = lax.axis_index('z') * 4 + lax.axis_index('y')
        inv_sqrt = lax.rsqrt(degree.astype(jnp.float32))[:, None]
        meta = jnp.stack([rep, core, zy]).astype(jnp.int32)

        half = jnp.concatenate([node_feat, degree.astype(bf)[:, None], jnp.zeros((nodes, 64 - f_in - 1), bf)], axis=1)
        packed = jnp.concatenate([half[:nodes // 2], half[nodes // 2:]], axis=1)
        packed = with_layout_constraint(packed, Layout((0, 1)))
        near = lax.all_gather(packed, ('z', 'y', 'core'), axis=0)
        feats = lax.all_gather(packed, ('rep', 'z', 'y', 'core'), axis=0).reshape(4, 32, nodes // 2, LANES)

        blk = nbr_col // (4 * nodes)
        inner = (blk // 2) * nodes + nbr_col % nodes
        lane_id = jnp.arange(4 * nodes)[:, None]
        pos_one = ((blk % 2) * (16 * nodes) + inner - lane_id % 4) * 2 + PAD
        pos_two = ((blk + core) % 2) * (16 * nodes) + inner - lane_id % 8 + PAD
        edge_wt = jnp.where(nbr_mask > 0, nbr_wt, jnp.zeros_like(nbr_wt))
        deg_own = degree.astype(bf).reshape(-1, 16, 8).transpose(0, 2, 1)
        deg_own = jnp.pad(deg_own, ((0, 0), (0, 0), (0, LANES - 16)), constant_values=1)

        def slot_major(pos):
            return pos.T.reshape(8, -1, LANES).transpose(1, 0, 2).reshape(-1)

        def by_core(x):
            y = lax.ppermute(x, 'core', swap)
            return jnp.stack([jnp.where(core == 0, x, y), jnp.where(core == 0, y, x)])

        idx_one = slot_major(pos_one)
        wt_q = jnp.repeat(edge_wt.reshape(-1, 16, 4, 8).transpose(0, 2, 1, 3).reshape(-1, 4, LANES), 2, axis=1)
        wt_one = jnp.concatenate([wt_q, deg_own], axis=0)
        idx_near, wt_near = by_core(idx_one).reshape(-1), by_core(wt_one).reshape(-1, 8, LANES)

        def with_far(x):
            parts = [x]
            for d in range(1, 4):
                parts.append(lax.ppermute(x, 'rep', [((t + d) % 4, t) for t in range(4)]))
            return jnp.concatenate(parts, axis=0)

        idx_one, wt_one = with_far(idx_near), with_far(wt_near)

        idx_own = slot_major(pos_two)
        wt_own = edge_wt.reshape(-1, 16, 8, 8).transpose(0, 2, 1, 3).reshape(-1, 8, LANES)
        idx_mine = lax.all_to_all(idx_own.reshape(4, -1), 'rep', 0, 0).reshape(-1)
        wt_mine = lax.all_to_all(wt_own.reshape(4, -1, 8, LANES), 'rep', 0, 0).reshape(-1, 8, LANES)
        feats, idx_one, wt_one, idx_mine, wt_mine = lax.optimization_barrier((feats, idx_one, wt_one, idx_mine, wt_mine))
        idx_two = lax.all_gather(idx_mine, ('z', 'y'), axis=0).reshape(-1)
        wt_two = lax.all_gather(jnp.concatenate([wt_mine, deg_own], axis=0), ('z', 'y'), axis=0).reshape(-1, 8, LANES)

        w_loc = lax.dynamic_slice_in_dim(w_one, (rep * 2 + core) * 256, 256, axis=1)
        wbd = jnp.zeros((LANES, 512), bf).at[:f_in, :256].set(w_loc).at[64:64 + f_in, 256:].set(w_loc)

        a = gather_call(Plan('one', (0,), 64, 2, True, False), meta, idx_near, wt_near, ((near,),), (wbd,))
        h = gather_call(Plan('one', (1, 3, 2), 64, 2, False, True), meta, idx_one, wt_one, ((feats,),), (wbd, a))
        h, idx_two, wt_two = lax.optimization_barrier((h, idx_two, wt_two))
        h = lax.all_to_all(h.reshape(8, nodes, 256), ('rep', 'core'), 0, 0)

        s_two = project_call(h, w_two, jnp.broadcast_to(inv_sqrt, (nodes, LANES)))
        t_0 = lax.all_to_all(s_two, ('z', 'y'), 0, 0)
        t_1, t_3 = (lax.ppermute(t_0, 'rep', shift[d]) for d in (1, 3))
        other = lambda t: lax.ppermute(t, 'core', swap)
        a = gather_call(Plan('two', (0,), 128, 1, True, False), meta, idx_two, wt_two, ((t_0, other(t_0)),))
        a, t_1, t_3 = lax.optimization_barrier((a, t_1, t_3))
        t_2 = [lax.ppermute(t_1[:8], 'rep', shift[1]), lax.ppermute(t_3[8:], 'rep', shift[3])]
        a = gather_call(Plan('two', (1, 3), 128, 1, False, False), meta, idx_two, wt_two, ((t_1, other(t_1)), (t_3, other(t_3))), (a,))
        a, *t_2 = lax.optimization_barrier((a, *t_2))
        w_pad = jnp.pad(w_three, ((0, 0), (0, LANES - cls)))
        a = a.reshape(16, 2, nodes // 2, LANES)
        far = (*t_2, *map(other, t_2))
        s_three = []
        for half in range(2):
            h = gather_call(Plan('two', (2,), 64, 1, False, True, half), meta, idx_two, wt_two, (far,), (a,))
            h = lax.all_to_all(h.reshape(16, nodes // 2, LANES), ('z', 'y'), 0, 0)
            h = h.transpose(1, 0, 2).reshape(nodes // 2, hid)
            scale = inv_sqrt[half * (nodes // 2):(half + 1) * (nodes // 2)]
            s_three.append((jnp.dot(h, w_pad, preferred_element_type=jnp.float32) * scale).astype(bf))
        s_three = jnp.concatenate(s_three, axis=0)
        s_all = lax.all_gather(s_three, ('z', 'y', 'core'), axis=0)
        part = gather_call(Plan('three', (0,), 32, 1, True, False), meta, idx_own, wt_own, ((s_all,),))
        neigh = lax.psum_scatter(part, 'rep', scatter_dimension=0, tiled=True)
        return (inv_sqrt * (neigh + s_three.astype(jnp.float32)))[:, :cls]

    rows = ('z', 'y', 'core')
    row_spec = P((*rows, 'rep'), None)
    table_spec = P(rows, 'rep')
    full = P(None, None)
    return jax.shard_map(network, mesh=mesh4, in_specs=(row_spec, P((*rows, 'rep')), table_spec, table_spec, table_spec, full, full, full),
                         out_specs=row_spec, check_vma=False)
```
